32 devices in a mesh: gx: 8 (over y, x, core), gy: 4 (over z).
Axes of the slice: x: 2, y: 2, z: 4, core: 2. Of those that a mesh axis runs over, the one named last changes fastest.
Arguments:
- signals: float32 [16, 32, 16, 128], P('gx', 'gy'), may hold values from -6 to 6
- tiles: bfloat16 [16, 32, 4, 128, 128], P('gx', 'gy'), may hold values from 0 to 0.00390625
- tile_dir: int32 [16, 32, 4], P('gx', 'gy'), may hold values from 0 to 8
- tile_mask: int32 [16, 32, 4], P('gx', 'gy'), may hold values 0 or 1
- live_rows: int32 [16, 32], P('gx', 'gy'), may hold values from 32 to 128
- bound_rows: int32 [16, 32], P('gx', 'gy'), may hold values from 1 to 32, as said below
- scale_coeffs: float32 [6, 5], replicated, may hold values from -1 to 1
- spectral_bound: float32 [1], replicated, may hold values from 2.5 to 4
Outputs:
- coefficients: float32 [6, 16, 32, 16, 128], P(None, 'gx', 'gy')
- energy: float32 [6, 16], replicated
The draws below stay inside these ranges and needn't reach their ends.
Inputs may be any that keep to these rules, and one draw needn't show every extreme that they name: `bound_rows`: in every draw, some blocks on every device have exactly 32 boundary rows.
All inputs are finite; a program needn't handle non-finite values. No bound on the sum of `tile_mask` on one device may be relied on, other than what follows from the above.
Results may differ from the reference program's by a relative error of at most 0.0003.
Values may be sent and summed in bfloat16 or wider, within the bound.
A program may use at most 64 MiB of HBM per device.

```python
import jax
import jax.numpy as jnp
from jax import lax

SIG = 16
SCALES = 6
DEG = 4
SLOTS = 4
TILE = 128
BMAX = 32
BY = 8
NBX = 16
NBY = 32


def draw_bound_rows(key, part):
    drawn = jax.random.randint(key, (NBX, NBY), 1, BMAX + 1, dtype=jnp.int32)
    columns = lax.broadcasted_iota(jnp.int32, (NBX, NBY), 1)
    return jnp.where(columns % BY == 0, jnp.int32(BMAX), drawn)


def with_ends(values, own_key, low, high):
    spot = [jax.random.randint(jax.random.fold_in(own_key, axis), (), 0, length) for axis, length in enumerate(values.shape)]
    main_axis = values.shape.index(max(values.shape))
    next_to = spot[:main_axis] + [(spot[main_axis] + 1) % values.shape[main_axis]] + spot[main_axis + 1:]
    return values.at[tuple(spot)].set(low).at[tuple(next_to)].set(high)


def steps_of(key, shape, cuts, low, high):
    def one(position, shards_of):
        steps = jax.random.uniform(jax.random.fold_in(jax.random.fold_in(key, 6), position), (shards_of,), jnp.float32, low / len(cuts), high / len(cuts))
        return jnp.repeat(jnp.exp(steps), shape[position] // shards_of).reshape((-1,) + (1,) * (len(shape) - position - 1))

    factor_of = one(*cuts[0])
    for cut in cuts[1:]:
        factor_of = factor_of * one(*cut)
    return factor_of


def scatter_about(key, dims, spread, limit, cuts=(), held_as=jnp.bfloat16):
    values = jax.random.normal(key, dims, jnp.float32) * spread
    if len(cuts) > 0:
        values = steps_of(key, dims, cuts, -0.22, 0.18) * values
    return jnp.clip(values, min=-limit, max=limit).astype(held_as)


def setup_inputs(seed: int = 0) -> dict:
    key_list = jax.random.split(jax.random.key(seed), 9)
    return {
        "signals": scatter_about(key_list[0], (NBX, NBY, SIG, TILE), 1.0, 6.0, ((0, 8), (1, 4)), jnp.float32),
        "tiles": jnp.clip(0.00390625 * jax.random.uniform(key_list[1], (NBX, NBY, SLOTS, TILE, TILE), jnp.float32) ** steps_of(key_list[1], (NBX, NBY, SLOTS, TILE, TILE), ((0, 8), (1, 4)), -0.2, 0.2), 0.0, 0.00390625).astype(jnp.bfloat16),
        "tile_dir": with_ends(jax.random.randint(key_list[2], (NBX, NBY, SLOTS), 0, 9), jax.random.fold_in(key_list[2], 1), 0, 8).astype(jnp.int32),
        "tile_mask": with_ends((jax.random.randint(key_list[3], (NBX, NBY, SLOTS), 0, 4) < 3).astype(jnp.int32), jax.random.fold_in(key_list[3], 1), 0, 1),
        "live_rows": with_ends(jax.random.randint(key_list[4], (NBX, NBY), TILE // 4, TILE + 1), jax.random.fold_in(key_list[4], 1), TILE // 4, TILE).astype(jnp.int32),
        "bound_rows": draw_bound_rows(jax.random.fold_in(key_list[8], 71), 0),
        "scale_coeffs": jnp.clip(jax.random.uniform(key_list[6], (SCALES, DEG + 1), jnp.float32, -1.0, 1.0), -1.0, 1.0),
        "spectral_bound": jnp.clip(jax.random.uniform(key_list[7], (1,), jnp.float32, 2.5, 4.0), 2.5, 4.0),
    }


def adjacency(values, tiles, tile_dir, tile_mask, bound_ind):
    own_rows = values.astype(jnp.bfloat16)
    edge_rows = (values * bound_ind[:, :, None, :]).astype(jnp.bfloat16)
    padded = jnp.pad(edge_rows, ((1, 1), (1, 1), (0, 0), (0, 0)))
    extent_x = values.shape[0]
    extent_y = values.shape[1]
    slot_list = []
    for slot_index in range(SLOTS):
        picked = jnp.zeros_like(own_rows)
        for direction in range(9):
            step_x = direction // 3 - 1
            step_y = direction % 3 - 1
            if direction == 4:
                source = own_rows
            else:
                source = padded[1 + step_x:1 + step_x + extent_x, 1 + step_y:1 + step_y + extent_y]
            matches = (tile_dir[:, :, slot_index] == direction)[:, :, None, None]
            picked = jnp.where(matches, source, picked)
        kept_mask = (tile_mask[:, :, slot_index] == 1)[:, :, None, None]
        picked = jnp.where(kept_mask, picked, jnp.zeros_like(picked))
        slot_list.append(picked)
    inputs = jnp.stack(slot_list, axis=2)

    def one_row(bundle):
        tile_row, input_row = bundle
        return jnp.einsum("jsrc,jsgc->jgr", tile_row.astype(jnp.float32), input_row.astype(jnp.float32))

    return lax.map(one_row, (tiles, inputs))


def scaled_laplacian(values, adjacent, degree, factor):
    return factor * (degree * values - adjacent) - values


def reference(signals, tiles, tile_dir, tile_mask, live_rows, bound_rows, scale_coeffs, spectral_bound):
    positions = lax.broadcasted_iota(jnp.int32, (1, 1, TILE), 2)
    live_ind = (positions < live_rows[:, :, None]).astype(jnp.float32)
    bound_ind = (positions < bound_rows[:, :, None]).astype(jnp.float32)
    initial = signals * live_ind[:, :, None, :]
    joined = jnp.concatenate([initial, live_ind[:, :, None, :]], axis=2)
    first_pass = adjacency(joined, tiles, tile_dir, tile_mask, bound_ind) * live_ind[:, :, None, :]
    degree = first_pass[:, :, SIG:, :]
    factor = 2.0 / spectral_bound[0]
    previous = initial
    current = scaled_laplacian(initial, first_pass[:, :, :SIG, :], degree, factor)
    totals = 0.5 * scale_coeffs[:, 0][:, None, None, None, None] * initial[None]
    totals = totals + scale_coeffs[:, 1][:, None, None, None, None] * current[None]
    for degree_index in range(2, DEG + 1):
        adjacent = adjacency(current, tiles, tile_dir, tile_mask, bound_ind) * live_ind[:, :, None, :]
        following = 2.0 * scaled_laplacian(current, adjacent, degree, factor) - previous
        previous = current
        current = following
        totals = totals + scale_coeffs[:, degree_index][:, None, None, None, None] * current[None]
    energy = jnp.sum(totals * totals, axis=(1, 2, 4)) / (NBX * NBY * TILE)
    return totals, energy
```

```python
import functools

import jax
import jax.numpy as jnp
from jax import lax
from jax.experimental import pallas as pl
from jax.experimental.pallas import tpu as pltpu
from jax.sharding import PartitionSpec as P

DEG = 4
EDGE = 32
MESH = pl.DeviceIdType.MESH
NT = (((1,), (1,)), ((), ()))


def kernel(
    nx, ny, sig, tiles_hbm, tdir, tmask, live_rows, bound_rows, coef, bound,
    totals, energy,
    tiles, w_own, w_edge, own0, own, acc, cheb, slope, en_all, pads,
    tile_sem, send_sem, recv_sem, en_send, en_recv,
):
    ex, ey, chan, size = sig.shape
    slots = tiles.shape[2]
    scales = coef.shape[0]
    groups = size // EDGE
    n = nx * ny
    gx, gy = lax.axis_index("gx"), lax.axis_index("gy")
    me = gx * ny + gy
    blocks = [(i, j) for i in range(ex) for j in range(ey)]

    for r in range(DEG):
        pad = pads[r]
        for row in (0, ex + 1, ex + 2):
            pad[row] = jnp.zeros(pad.shape[1:], pad.dtype)
        for row in range(1, ex + 1):
            for col in (0, ey + 1):
                pad[row, col] = jnp.zeros(pad.shape[2:], pad.dtype)

    barrier = pltpu.get_barrier_semaphore()

    @pl.loop(1, n)
    def _(k):
        peer = lax.rem(me + k, n)
        pl.semaphore_signal(
            barrier, inc=1, device_id=(peer // ny, lax.rem(peer, ny)), device_id_type=MESH
        )

    def tile_copy(i, j):
        return pltpu.make_async_copy(
            tiles_hbm.at[i, j], tiles.at[i, j], tile_sem.at[i * ey + j]
        )

    for i, j in blocks:
        tile_copy(i, j).start()

    lane = lax.broadcasted_iota(jnp.int32, (1, size), 1)
    factor = 2.0 / jnp.full((1, size), bound[0], jnp.float32)

    def live_of(i, j):
        return (lane < live_rows[i, j]).astype(jnp.float32)

    def edge_of(i, j):
        return (lane < bound_rows[i, j]).astype(jnp.float32)

    def spread(v, i, j):
        v = v * edge_of(i, j)
        step = EDGE
        while step < size:
            v = v + pltpu.roll(v, step, 1)
            step *= 2
        return v.astype(jnp.bfloat16)

    first_row = lax.broadcasted_iota(jnp.int32, (chan, size), 0) == 0
    for b, (i, j) in enumerate(blocks):
        live = live_of(i, j)
        v = sig[i, j] * live
        cheb[0, b] = v
        ind = jnp.where(first_row, jnp.broadcast_to(live, (chan, size)), 0.0)
        joined = jnp.concatenate([v, ind], axis=0)
        own0[b] = joined.astype(jnp.bfloat16)
        pads[0][i + 1, j + 1] = spread(joined, i, j)

    pl.semaphore_wait(barrier, n - 1)

    sides = []
    for dx in (-1, 0, 1):
        for dy in (-1, 0, 1):
            if dx or dy:
                sides.append((dx, dy))

    def cut(d, extent, far):
        if d == 0:
            return pl.ds(1, extent)
        if far:
            return pl.ds(extent + 1 if d < 0 else 0, 1)
        return pl.ds(1 if d < 0 else extent, 1)

    def inside(dx, dy):
        ok = None
        for d, g, m in ((dx, gx, nx), (dy, gy, ny)):
            if d:
                here = g > 0 if d < 0 else g < m - 1
                ok = here if ok is None else jnp.logical_and(ok, here)
        return ok

    def halo(r, k, dx, dy):
        pad = pads[r]
        return pltpu.make_async_remote_copy(
            src_ref=pad.at[cut(dx, ex, False), cut(dy, ey, False)],
            dst_ref=pad.at[cut(dx, ex, True), cut(dy, ey, True)],
            send_sem=send_sem.at[r, k],
            recv_sem=recv_sem.at[r, k],
            device_id=(gx + dx, gy + dy),
            device_id_type=MESH,
        )

    order = sorted(range(len(sides)), key=lambda k: -abs(sides[k][0]) - abs(sides[k][1]))

    def send(r):
        for k in order:
            dx, dy = sides[k]

            @pl.when(inside(dx, dy))
            def _():
                halo(r, k, dx, dy).start()

    def receive(r):
        for k in order:
            dx, dy = sides[k]

            @pl.when(inside(-dx, -dy))
            def _():
                halo(r, k, dx, dy).wait_recv()

    def add_totals(k):
        for s in range(scales):
            c = coef[s, k] * (0.5 if k == 0 else 1.0)
            for b, (i, j) in enumerate(blocks):
                term = c * cheb[k, b]
                totals[s, i, j] = term if k == 0 else totals[s, i, j] + term

    def weights(i, j):
        b = i * ey + j
        total = None
        packed = None
        for s in range(slots):
            tile = tiles[i, j, s].astype(jnp.float32)
            used = jnp.logical_and(tmask[i, s, j] == 1, tdir[i, s, j] == 4)
            term = tile * jnp.where(used, 1.0, 0.0)
            total = term if total is None else total + term
            rolled = pltpu.roll(tile, s * EDGE, 1) if s else tile
            packed = rolled if packed is None else jnp.where(lane >= s * EDGE, rolled, packed)
        high = total.astype(jnp.bfloat16)
        w_own[b, :, :size] = high
        w_own[b, :, size:] = (total - high.astype(jnp.float32)).astype(jnp.bfloat16)
        w_edge[b] = packed.astype(jnp.bfloat16)

    def gather(r, i, j):
        pad = pads[r]
        picked = None
        for s in range(slots):
            d = tdir[i, s, j]
            ok = jnp.logical_and(tmask[i, s, j] == 1, d != 4)
            row = (d * 11) >> 5
            col = d - 3 * row
            cell = pad[jnp.where(ok, row + i, ex + 2), jnp.where(ok, col + j, 0)]
            group = jnp.logical_and(lane >= s * EDGE, lane < (s + 1) * EDGE)
            term = cell * group.astype(jnp.bfloat16)
            picked = term if picked is None else picked + term
        return picked

    for r in range(DEG):
        send(r)
        add_totals(r)
        for b, (i, j) in enumerate(blocks):
            if r == 0:
                tile_copy(i, j).wait()
                weights(i, j)
            mine = own0[b] if r == 0 else own[r - 1, b]
            acc[b, : mine.shape[0]] = lax.dot_general(
                jnp.concatenate([mine, mine], axis=1), w_own[b], NT,
                preferred_element_type=jnp.float32,
            )
        receive(r)
        for b, (i, j) in enumerate(blocks):
            rows = 2 * chan if r == 0 else chan
            adj = acc[b, :rows] + lax.dot_general(
                gather(r, i, j), w_edge[b], NT, preferred_element_type=jnp.float32
            )
            scale = factor * live_of(i, j)
            v = cheb[r, b]
            if r == 0:
                slope[b] = scale * adj[chan : chan + 1] - 1.0
                following = slope[b] * v - scale * adj[:chan]
            else:
                following = 2.0 * (slope[b] * v - scale * adj) - cheb[r - 1, b]
            cheb[r + 1, b] = following
            if r < DEG - 1:
                own[r, b] = following.astype(jnp.bfloat16)
                pads[r + 1][i + 1, j + 1] = spread(following, i, j)

    sums = []
    for s in range(scales):
        c = coef[s, DEG]
        part = jnp.zeros((chan, size), jnp.float32)
        for b, (i, j) in enumerate(blocks):
            t = totals[s, i, j] + c * cheb[DEG, b]
            totals[s, i, j] = t
            part = part + t * t
        sums.append(part)

    width = en_all.shape[2]
    if width > scales * chan:
        sums.append(jnp.zeros((width - scales * chan, size), jnp.float32))
    local = lax.dot_general(
        jnp.ones((8, size), jnp.float32), jnp.concatenate(sums, axis=0), NT,
        precision=lax.Precision.HIGHEST, preferred_element_type=jnp.float32,
    )
    en_all[me] = local[:1]

    def share(k, slot):
        peer = lax.rem(me + k, n)
        return pltpu.make_async_remote_copy(
            src_ref=en_all.at[slot],
            dst_ref=en_all.at[slot],
            send_sem=en_send.at[k],
            recv_sem=en_recv.at[slot],
            device_id=(peer // ny, lax.rem(peer, ny)),
            device_id_type=MESH,
        )

    @pl.loop(1, n)
    def _(k):
        share(k, me).start()

    @pl.loop(1, n)
    def _(k):
        share(k, lax.rem(me + k, n)).wait_recv()

    total = jnp.sum(en_all[...], axis=0) * (1.0 / (ex * ey * size * n))
    for s in range(scales):
        energy[s : s + 1, :] = total[:, s * chan : (s + 1) * chan]

    @pl.loop(1, n)
    def _(k):
        share(k, me).wait_send()

    for r in range(DEG):
        for k in order:
            dx, dy = sides[k]

            @pl.when(inside(dx, dy))
            def _():
                halo(r, k, dx, dy).wait_send()


def solution(mesh):
    nx, ny = mesh.shape["gx"], mesh.shape["gy"]
    n = nx * ny

    def shards(
        signals, tiles, tile_dir, tile_mask, live_rows, bound_rows, scale_coeffs, spectral_bound
    ):
        ex, ey, chan, size = signals.shape
        slots = tiles.shape[2]
        scales = scale_coeffs.shape[0]
        nb = ex * ey
        width = -(-scales * chan // 128) * 128
        bf, f32 = jnp.bfloat16, jnp.float32
        vmem = pl.BlockSpec(memory_space=pltpu.VMEM)
        smem = pl.BlockSpec(memory_space=pltpu.SMEM)
        hbm = pl.BlockSpec(memory_space=pltpu.HBM)
        return pl.pallas_call(
            functools.partial(kernel, nx, ny),
            out_shape=(
                jax.ShapeDtypeStruct((scales, ex, ey, chan, size), f32),
                jax.ShapeDtypeStruct((scales, chan), f32),
            ),
            in_specs=[vmem, hbm] + [smem] * 6,
            out_specs=(vmem, vmem),
            scratch_shapes=[
                pltpu.VMEM((ex, ey, slots, size, size), bf),
                pltpu.VMEM((nb, size, 2 * size), bf),
                pltpu.VMEM((nb, size, size), bf),
                pltpu.VMEM((nb, 2 * chan, size), bf),
                pltpu.VMEM((DEG - 1, nb, chan, size), bf),
                pltpu.VMEM((nb, 2 * chan, size), f32),
                pltpu.VMEM((DEG + 1, nb, chan, size), f32),
                pltpu.VMEM((nb, 1, size), f32),
                pltpu.VMEM((n, 1, width), f32),
                [
                    pltpu.VMEM((ex + 3, ey + 2, chan * (2 if r == 0 else 1), size), bf)
                    for r in range(DEG)
                ],
                pltpu.SemaphoreType.DMA((nb,)),
                pltpu.SemaphoreType.DMA((DEG, 8)),
                pltpu.SemaphoreType.DMA((DEG, 8)),
                pltpu.SemaphoreType.DMA((n,)),
                pltpu.SemaphoreType.DMA((n,)),
            ],
            compiler_params=pltpu.CompilerParams(
                collective_id=0, has_side_effects=True, vmem_limit_bytes=40 * 1024 * 1024
            ),
        )(
            signals, tiles, jnp.swapaxes(tile_dir, 1, 2), jnp.swapaxes(tile_mask, 1, 2),
            live_rows, bound_rows, scale_coeffs, spectral_bound,
        )

    placed = (
        P("gx", "gy", None, None),
        P("gx", "gy", None, None, None),
        P("gx", "gy", None),
        P("gx", "gy", None),
        P("gx", "gy"),
        P("gx", "gy"),
        P(),
        P(),
    )
    return jax.shard_map(
        shards,
        mesh=mesh,
        in_specs=placed,
        out_specs=(P(None, "gx", "gy", None, None), P()),
        check_vma=False,
    )
```

```python
import functools

import jax
import jax.numpy as jnp
from jax import lax
from jax.experimental import pallas as pl
from jax.experimental.pallas import tpu as pltpu
from jax.sharding import PartitionSpec as P

DEG = 4
VMEM_LIMIT = 67043328
EDGE = 32
MESH = pl.DeviceIdType.MESH
NT = (((1,), (1,)), ((), ()))


def kernel(
    nx, ny, sig_hbm, tiles_hbm, tdir_hbm, tmask_hbm, live_hbm, edge_hbm, coef_hbm, bound_hbm,
    totals, energy,
    sig, tdir, tmask, live_rows, bound_rows, coef, bound, tiles, w_own, w_edge, own0, own, acc, cheb, slope, en_all, pads,
    tile_sem, send_sem, recv_sem, en_send, en_recv, in_sem,
):
    ex, ey, chan, size = sig.shape
    slots = tiles.shape[2]
    scales = coef.shape[0]
    groups = size // EDGE
    n = nx * ny
    gx, gy = lax.axis_index("gx"), lax.axis_index("gy")
    me = gx * ny + gy
    blocks = [(i, j) for i in range(ex) for j in range(ey)]

    for r in range(DEG):
        pad = pads[r]
        for row in (0, ex + 1, ex + 2):
            pad[row] = jnp.zeros(pad.shape[1:], pad.dtype)
        for row in range(1, ex + 1):
            for col in (0, ey + 1):
                pad[row, col] = jnp.zeros(pad.shape[2:], pad.dtype)

    barrier = pltpu.get_barrier_semaphore()

    fetches = [
        pltpu.make_async_copy(src, dst, in_sem.at[k])
        for k, (src, dst) in enumerate(
            [
                (live_hbm, live_rows), (edge_hbm, bound_rows), (sig_hbm, sig), (tdir_hbm, tdir),
                (tmask_hbm, tmask), (coef_hbm, coef), (bound_hbm, bound),
            ]
        )
    ]
    for copy in fetches:
        copy.start()

    def others(act):
        def one(kx, px, ky):
            py = gy + ky
            act(kx * ny + ky, px, jnp.where(py >= ny, py - ny, py))

        for ky in range(1, ny):
            one(0, gx, ky)

        @pl.loop(1, nx)
        def _(kx):
            px = gx + kx
            px = jnp.where(px >= nx, px - nx, px)
            for ky in range(ny):
                one(kx, px, ky)

    def greet(k, px, py):
        pl.semaphore_signal(barrier, inc=1, device_id=(px, py), device_id_type=MESH)

    others(greet)

    def tile_copy(i, j):
        return pltpu.make_async_copy(
            tiles_hbm.at[i, j], tiles.at[i, j], tile_sem.at[i * ey + j]
        )

    for i, j in blocks:
        tile_copy(i, j).start()

    for copy in fetches:
        copy.wait()

    lane = lax.broadcasted_iota(jnp.int32, (1, size), 1)
    factor = 2.0 / jnp.full((1, size), bound[0, 0], jnp.float32)

    def live_of(i, j):
        return (lane < live_rows[i, j]).astype(jnp.float32)

    def edge_of(i, j):
        return (lane < bound_rows[i, j]).astype(jnp.float32)

    def spread(v, i, j):
        v = v * edge_of(i, j)
        step = EDGE
        while step < size:
            v = v + pltpu.roll(v, step, 1)
            step *= 2
        return v.astype(jnp.bfloat16)

    first_row = lax.broadcasted_iota(jnp.int32, (chan, size), 0) == 0
    for b, (i, j) in enumerate(blocks):
        live = live_of(i, j)
        v = sig[i, j] * live
        cheb[0, b] = v
        ind = jnp.where(first_row, jnp.broadcast_to(live, (chan, size)), 0.0)
        joined = jnp.concatenate([v, ind], axis=0)
        own0[b] = joined.astype(jnp.bfloat16)
        pads[0][i + 1, j + 1] = spread(joined, i, j)

    pl.semaphore_wait(barrier, n - 1)

    sides = []
    for dx in (-1, 0, 1):
        for dy in (-1, 0, 1):
            if dx or dy:
                sides.append((dx, dy))

    def cut(d, extent, far):
        if d == 0:
            return pl.ds(1, extent)
        if far:
            return pl.ds(extent + 1 if d < 0 else 0, 1)
        return pl.ds(1 if d < 0 else extent, 1)

    def inside(dx, dy):
        ok = None
        for d, g, m in ((dx, gx, nx), (dy, gy, ny)):
            if d:
                here = g > 0 if d < 0 else g < m - 1
                ok = here if ok is None else jnp.logical_and(ok, here)
        return ok

    def halo(r, k, dx, dy):
        pad = pads[r]
        return pltpu.make_async_remote_copy(
            src_ref=pad.at[cut(dx, ex, False), cut(dy, ey, False)],
            dst_ref=pad.at[cut(dx, ex, True), cut(dy, ey, True)],
            send_sem=send_sem.at[r, k],
            recv_sem=recv_sem.at[r, k],
            device_id=(gx + dx, gy + dy),
            device_id_type=MESH,
        )

    order = sorted(range(len(sides)), key=lambda k: -abs(sides[k][0]) - abs(sides[k][1]))
    corners = [(i, j) for i, j in blocks if i in (0, ex - 1) and j in (0, ey - 1)]
    inner = [(i, j) for i, j in blocks if (i, j) not in corners]

    def send(r, chosen):
        for k in order:
            dx, dy = sides[k]
            if not chosen(dx, dy):
                continue

            @pl.when(inside(dx, dy))
            def _():
                halo(r, k, dx, dy).start()

    def receive(r):
        for k in order:
            dx, dy = sides[k]

            @pl.when(inside(-dx, -dy))
            def _():
                halo(r, k, dx, dy).wait_recv()

    def add_totals(k):
        for s in range(scales):
            c = coef[s, k] * (0.5 if k == 0 else 1.0)
            for b, (i, j) in enumerate(blocks):
                term = c * cheb[k, b]
                totals[s, i, j] = term if k == 0 else totals[s, i, j] + term

    def weights(i, j):
        b = i * ey + j
        total = None
        packed = None
        for s in range(slots):
            tile = tiles[i, j, s].astype(jnp.float32)
            used = jnp.logical_and(tmask[i, s, j] == 1, tdir[i, s, j] == 4)
            term = tile * jnp.where(used, 1.0, 0.0)
            total = term if total is None else total + term
            rolled = pltpu.roll(tile, s * EDGE, 1) if s else tile
            packed = rolled if packed is None else jnp.where(lane >= s * EDGE, rolled, packed)
        high = total.astype(jnp.bfloat16)
        w_own[b, :, :size] = high
        w_own[b, :, size:] = (total - high.astype(jnp.float32)).astype(jnp.bfloat16)
        w_edge[b] = packed.astype(jnp.bfloat16)

    def gather(r, i, j):
        pad = pads[r]
        picked = None
        for s in range(slots):
            d = tdir[i, s, j]
            ok = jnp.logical_and(tmask[i, s, j] == 1, d != 4)
            row = (d * 11) >> 5
            col = d - 3 * row
            cell = pad[jnp.where(ok, row + i, ex + 2), jnp.where(ok, col + j, 0)]
            group = jnp.logical_and(lane >= s * EDGE, lane < (s + 1) * EDGE)
            term = cell * group.astype(jnp.bfloat16)
            picked = term if picked is None else picked + term
        return picked

    send(0, lambda dx, dy: True)
    for r in range(DEG):
        add_totals(r)
        for b, (i, j) in enumerate(blocks):
            if r == 0:
                tile_copy(i, j).wait()
                weights(i, j)
            mine = own0[b] if r == 0 else own[r - 1, b]
            acc[b, : mine.shape[0]] = lax.dot_general(
                jnp.concatenate([mine, mine], axis=1), w_own[b], NT,
                preferred_element_type=jnp.float32,
            )
        receive(r)
        for i, j in corners + inner:
            b = i * ey + j
            rows = 2 * chan if r == 0 else chan
            adj = acc[b, :rows] + lax.dot_general(
                gather(r, i, j), w_edge[b], NT, preferred_element_type=jnp.float32
            )
            scale = factor * live_of(i, j)
            v = cheb[r, b]
            if r == 0:
                slope[b] = scale * adj[chan : chan + 1] - 1.0
                following = slope[b] * v - scale * adj[:chan]
            else:
                following = 2.0 * (slope[b] * v - scale * adj) - cheb[r - 1, b]
            cheb[r + 1, b] = following
            if r < DEG - 1:
                own[r, b] = following.astype(jnp.bfloat16)
                pads[r + 1][i + 1, j + 1] = spread(following, i, j)
                if (i, j) == corners[-1]:
                    send(r + 1, lambda dx, dy: dx and dy)
                if (i, j) == inner[-1]:
                    send(r + 1, lambda dx, dy: not (dx and dy))

    sums = []
    for s in range(scales):
        c = coef[s, DEG]
        part = jnp.zeros((chan, size), jnp.float32)
        for b, (i, j) in enumerate(blocks):
            t = totals[s, i, j] + c * cheb[DEG, b]
            totals[s, i, j] = t
            part = part + t * t
        sums.append(part)

    width = en_all.shape[2]
    if width > scales * chan:
        sums.append(jnp.zeros((width - scales * chan, size), jnp.float32))
    local = lax.dot_general(
        jnp.ones((8, size), jnp.float32), jnp.concatenate(sums, axis=0), NT,
        precision=lax.Precision.HIGHEST, preferred_element_type=jnp.float32,
    )
    en_all[me] = local[:1]

    def share(k, slot, px, py):
        return pltpu.make_async_remote_copy(
            src_ref=en_all.at[slot],
            dst_ref=en_all.at[slot],
            send_sem=en_send.at[k],
            recv_sem=en_recv.at[slot],
            device_id=(px, py),
            device_id_type=MESH,
        )

    others(lambda k, px, py: share(k, me, px, py).start())
    others(lambda k, px, py: share(k, px * ny + py, px, py).wait_recv())

    total = jnp.sum(en_all[...], axis=0) * (1.0 / (ex * ey * size * n))
    for s in range(scales):
        energy[s : s + 1, :] = total[:, s * chan : (s + 1) * chan]

    others(lambda k, px, py: share(k, me, px, py).wait_send())

    for r in range(DEG):
        for k in order:
            dx, dy = sides[k]

            @pl.when(inside(dx, dy))
            def _():
                halo(r, k, dx, dy).wait_send()


def solution(mesh):
    nx, ny = mesh.shape["gx"], mesh.shape["gy"]
    n = nx * ny

    def shards(
        signals, tiles, tile_dir, tile_mask, live_rows, bound_rows, scale_coeffs, spectral_bound
    ):
        ex, ey, chan, size = signals.shape
        slots = tiles.shape[2]
        scales = scale_coeffs.shape[0]
        nb = ex * ey
        width = -(-scales * chan // 128) * 128
        bf, f32 = jnp.bfloat16, jnp.float32
        vmem = pl.BlockSpec(memory_space=pltpu.VMEM)
        hbm = pl.BlockSpec(memory_space=pltpu.HBM)
        return pl.pallas_call(
            functools.partial(kernel, nx, ny),
            out_shape=(
                jax.ShapeDtypeStruct((scales, ex, ey, chan, size), f32),
                jax.ShapeDtypeStruct((scales, chan), f32),
            ),
            in_specs=[hbm] * 8,
            out_specs=(vmem, vmem),
            scratch_shapes=[
                pltpu.VMEM(signals.shape, f32),
                pltpu.SMEM((ex, slots, ey), jnp.int32),
                pltpu.SMEM((ex, slots, ey), jnp.int32),
                pltpu.SMEM((ex, ey), jnp.int32),
                pltpu.SMEM((ex, ey), jnp.int32),
                pltpu.SMEM(scale_coeffs.shape, f32),
                pltpu.SMEM((1, 1), f32),
                pltpu.VMEM((ex, ey, slots, size, size), bf),
                pltpu.VMEM((nb, size, 2 * size), bf),
                pltpu.VMEM((nb, size, size), bf),
                pltpu.VMEM((nb, 2 * chan, size), bf),
                pltpu.VMEM((DEG - 1, nb, chan, size), bf),
                pltpu.VMEM((nb, 2 * chan, size), f32),
                pltpu.VMEM((DEG + 1, nb, chan, size), f32),
                pltpu.VMEM((nb, 1, size), f32),
                pltpu.VMEM((n, 1, width), f32),
                [
                    pltpu.VMEM((ex + 3, ey + 2, chan * (2 if r == 0 else 1), size), bf)
                    for r in range(DEG)
                ],
                pltpu.SemaphoreType.DMA((nb,)),
                pltpu.SemaphoreType.DMA((DEG, 8)),
                pltpu.SemaphoreType.DMA((DEG, 8)),
                pltpu.SemaphoreType.DMA((n,)),
                pltpu.SemaphoreType.DMA((n,)),
                pltpu.SemaphoreType.DMA((8,)),
            ],
            compiler_params=pltpu.CompilerParams(
                collective_id=0, has_side_effects=True, vmem_limit_bytes=VMEM_LIMIT
            ),
        )(
            signals, tiles, jnp.swapaxes(tile_dir, 1, 2), jnp.swapaxes(tile_mask, 1, 2),
            live_rows, bound_rows, scale_coeffs, spectral_bound.reshape(1, 1),
        )

    placed = (
        P("gx", "gy", None, None),
        P("gx", "gy", None, None, None),
        P("gx", "gy", None),
        P("gx", "gy", None),
        P("gx", "gy"),
        P("gx", "gy"),
        P(),
        P(),
    )
    return jax.shard_map(
        shards,
        mesh=mesh,
        in_specs=placed,
        out_specs=(P(None, "gx", "gy", None, None), P()),
        check_vma=False,
    )
```

```python
import functools

import jax
import jax.numpy as jnp
from jax import lax
from jax.experimental import pallas as pl
from jax.experimental.pallas import tpu as pltpu
from jax.sharding import PartitionSpec as P

DEG = 4
VMEM_LIMIT = 67043328
EDGE = 32
MESH = pl.DeviceIdType.MESH
NT = (((1,), (1,)), ((), ()))


def kernel(
    nx, ny, sig_hbm, tiles_hbm, tdir_hbm, tmask_hbm, live_hbm, edge_hbm, coef_hbm, bound_hbm,
    totals_hbm, energy,
    totals, sig, tdir, tmask, live_rows, bound_rows, coef, bound, tiles, w_own, w_edge, own0, own, acc, cheb, slope, en_all, pads,
    tile_sem, send_sem, recv_sem, en_send, en_recv, in_sem, out_sem,
):
    ex, ey, chan, size = sig.shape
    slots = tiles.shape[2]
    scales = coef.shape[0]
    groups = size // EDGE
    n = nx * ny
    gx, gy = lax.axis_index("gx"), lax.axis_index("gy")
    me = gx * ny + gy
    blocks = [(i, j) for i in range(ex) for j in range(ey)]

    for r in range(DEG):
        pad = pads[r]
        for row in (0, ex + 1, ex + 2):
            pad[row] = jnp.zeros(pad.shape[1:], pad.dtype)
        for row in range(1, ex + 1):
            for col in (0, ey + 1):
                pad[row, col] = jnp.zeros(pad.shape[2:], pad.dtype)

    barrier = pltpu.get_barrier_semaphore()

    fetches = [
        pltpu.make_async_copy(src, dst, in_sem.at[k])
        for k, (src, dst) in enumerate(
            [
                (live_hbm, live_rows), (edge_hbm, bound_rows), (sig_hbm, sig), (tdir_hbm, tdir),
                (tmask_hbm, tmask), (coef_hbm, coef), (bound_hbm, bound),
            ]
        )
    ]
    for copy in fetches:
        copy.start()

    def others(act):
        def one(kx, px, ky):
            py = gy + ky
            act(kx * ny + ky, px, jnp.where(py >= ny, py - ny, py))

        for ky in range(1, ny):
            one(0, gx, ky)

        @pl.loop(1, nx)
        def _(kx):
            px = gx + kx
            px = jnp.where(px >= nx, px - nx, px)
            for ky in range(ny):
                one(kx, px, ky)

    def greet(k, px, py):
        pl.semaphore_signal(barrier, inc=1, device_id=(px, py), device_id_type=MESH)

    others(greet)

    def tile_copy(i, j):
        return pltpu.make_async_copy(
            tiles_hbm.at[i, j], tiles.at[i, j], tile_sem.at[i * ey + j]
        )

    for i, j in blocks:
        tile_copy(i, j).start()

    for copy in fetches:
        copy.wait()

    lane = lax.broadcasted_iota(jnp.int32, (1, size), 1)
    factor = 2.0 / jnp.full((1, size), bound[0, 0], jnp.float32)

    def live_of(i, j):
        return (lane < live_rows[i, j]).astype(jnp.float32)

    def edge_of(i, j):
        return (lane < bound_rows[i, j]).astype(jnp.float32)

    def spread(v, i, j):
        v = v * edge_of(i, j)
        step = EDGE
        while step < size:
            v = v + pltpu.roll(v, step, 1)
            step *= 2
        return v.astype(jnp.bfloat16)

    first_row = lax.broadcasted_iota(jnp.int32, (chan, size), 0) == 0
    for b, (i, j) in enumerate(blocks):
        live = live_of(i, j)
        v = sig[i, j] * live
        cheb[0, b] = v
        ind = jnp.where(first_row, jnp.broadcast_to(live, (chan, size)), 0.0)
        joined = jnp.concatenate([v, ind], axis=0)
        own0[b] = joined.astype(jnp.bfloat16)
        pads[0][i + 1, j + 1] = spread(joined, i, j)

    pl.semaphore_wait(barrier, n - 1)

    sides = []
    for dx in (-1, 0, 1):
        for dy in (-1, 0, 1):
            if dx or dy:
                sides.append((dx, dy))

    def cut(d, extent, far):
        if d == 0:
            return pl.ds(1, extent)
        if far:
            return pl.ds(extent + 1 if d < 0 else 0, 1)
        return pl.ds(1 if d < 0 else extent, 1)

    def inside(dx, dy):
        ok = None
        for d, g, m in ((dx, gx, nx), (dy, gy, ny)):
            if d:
                here = g > 0 if d < 0 else g < m - 1
                ok = here if ok is None else jnp.logical_and(ok, here)
        return ok

    def halo(r, k, dx, dy):
        pad = pads[r]
        return pltpu.make_async_remote_copy(
            src_ref=pad.at[cut(dx, ex, False), cut(dy, ey, False)],
            dst_ref=pad.at[cut(dx, ex, True), cut(dy, ey, True)],
            send_sem=send_sem.at[r, k],
            recv_sem=recv_sem.at[r, k],
            device_id=(gx + dx, gy + dy),
            device_id_type=MESH,
        )

    order = sorted(range(len(sides)), key=lambda k: -abs(sides[k][0]) - abs(sides[k][1]))
    corners = [(i, j) for i, j in blocks if i in (0, ex - 1) and j in (0, ey - 1)]
    inner = [(i, j) for i, j in blocks if (i, j) not in corners]

    def send(r, chosen):
        for k in order:
            dx, dy = sides[k]
            if not chosen(dx, dy):
                continue

            @pl.when(inside(dx, dy))
            def _():
                halo(r, k, dx, dy).start()

    def receive(r):
        for k in order:
            dx, dy = sides[k]

            @pl.when(inside(-dx, -dy))
            def _():
                halo(r, k, dx, dy).wait_recv()

    def add_totals(k):
        for s in range(scales):
            c = coef[s, k] * (0.5 if k == 0 else 1.0)
            for b, (i, j) in enumerate(blocks):
                term = c * cheb[k, b]
                totals[s, i, j] = term if k == 0 else totals[s, i, j] + term

    def weights(i, j):
        b = i * ey + j
        total = None
        packed = None
        for s in range(slots):
            tile = tiles[i, j, s].astype(jnp.float32)
            used = jnp.logical_and(tmask[i, s, j] == 1, tdir[i, s, j] == 4)
            term = tile * jnp.where(used, 1.0, 0.0)
            total = term if total is None else total + term
            rolled = pltpu.roll(tile, s * EDGE, 1) if s else tile
            packed = rolled if packed is None else jnp.where(lane >= s * EDGE, rolled, packed)
        high = total.astype(jnp.bfloat16)
        w_own[b, :, :size] = high
        w_own[b, :, size:] = (total - high.astype(jnp.float32)).astype(jnp.bfloat16)
        w_edge[b] = packed.astype(jnp.bfloat16)

    def gather(r, i, j):
        pad = pads[r]
        picked = None
        for s in range(slots):
            d = tdir[i, s, j]
            ok = jnp.logical_and(tmask[i, s, j] == 1, d != 4)
            row = (d * 11) >> 5
            col = d - 3 * row
            cell = pad[jnp.where(ok, row + i, ex + 2), jnp.where(ok, col + j, 0)]
            group = jnp.logical_and(lane >= s * EDGE, lane < (s + 1) * EDGE)
            term = cell * group.astype(jnp.bfloat16)
            picked = term if picked is None else picked + term
        return picked

    send(0, lambda dx, dy: True)
    for r in range(DEG):
        add_totals(r)
        for b, (i, j) in enumerate(blocks):
            if r == 0:
                tile_copy(i, j).wait()
                weights(i, j)
            mine = own0[b] if r == 0 else own[r - 1, b]
            acc[b, : mine.shape[0]] = lax.dot_general(
                jnp.concatenate([mine, mine], axis=1), w_own[b], NT,
                preferred_element_type=jnp.float32,
            )
        receive(r)
        for i, j in corners + inner:
            b = i * ey + j
            rows = 2 * chan if r == 0 else chan
            adj = acc[b, :rows] + lax.dot_general(
                gather(r, i, j), w_edge[b], NT, preferred_element_type=jnp.float32
            )
            scale = factor * live_of(i, j)
            v = cheb[r, b]
            if r == 0:
                slope[b] = scale * adj[chan : chan + 1] - 1.0
                following = slope[b] * v - scale * adj[:chan]
            else:
                following = 2.0 * (slope[b] * v - scale * adj) - cheb[r - 1, b]
            cheb[r + 1, b] = following
            if r < DEG - 1:
                own[r, b] = following.astype(jnp.bfloat16)
                pads[r + 1][i + 1, j + 1] = spread(following, i, j)
                if (i, j) == corners[-1]:
                    send(r + 1, lambda dx, dy: dx and dy)
                if (i, j) == inner[-1]:
                    send(r + 1, lambda dx, dy: not (dx and dy))

    def out_copy(s):
        return pltpu.make_async_copy(totals.at[s], totals_hbm.at[s], out_sem.at[s])

    sums = []
    for s in range(scales):
        c = coef[s, DEG]
        part = jnp.zeros((chan, size), jnp.float32)
        for b, (i, j) in enumerate(blocks):
            t = totals[s, i, j] + c * cheb[DEG, b]
            totals[s, i, j] = t
            part = part + t * t
        sums.append(part)
        out_copy(s).start()

    width = en_all.shape[2]
    if width > scales * chan:
        sums.append(jnp.zeros((width - scales * chan, size), jnp.float32))
    local = lax.dot_general(
        jnp.ones((8, size), jnp.float32), jnp.concatenate(sums, axis=0), NT,
        precision=lax.Precision.HIGHEST, preferred_element_type=jnp.float32,
    )
    en_all[me] = local[:1]

    def share(k, slot, px, py):
        return pltpu.make_async_remote_copy(
            src_ref=en_all.at[slot],
            dst_ref=en_all.at[slot],
            send_sem=en_send.at[k],
            recv_sem=en_recv.at[slot],
            device_id=(px, py),
            device_id_type=MESH,
        )

    others(lambda k, px, py: share(k, me, px, py).start())
    others(lambda k, px, py: share(k, px * ny + py, px, py).wait_recv())

    total = jnp.sum(en_all[...], axis=0) * (1.0 / (ex * ey * size * n))
    for s in range(scales):
        energy[s : s + 1, :] = total[:, s * chan : (s + 1) * chan]

    others(lambda k, px, py: share(k, me, px, py).wait_send())

    for r in range(DEG):
        for k in order:
            dx, dy = sides[k]

            @pl.when(inside(dx, dy))
            def _():
                halo(r, k, dx, dy).wait_send()

    for s in range(scales):
        out_copy(s).wait()


def hand_out(made_hbm, energy_in, out_hbm, energy_out, held, held_energy, load_sem, store_sem):
    count = held.shape[0]
    loads = [
        pltpu.make_async_copy(made_hbm.at[s], held.at[s], load_sem.at[s]) for s in range(count)
    ] + [pltpu.make_async_copy(energy_in, held_energy, load_sem.at[count])]
    stores = [
        pltpu.make_async_copy(held.at[s], out_hbm.at[s], store_sem.at[s]) for s in range(count)
    ] + [pltpu.make_async_copy(held_energy, energy_out, store_sem.at[count])]
    for load in loads:
        load.start()
    for load, store in zip(loads, stores):
        load.wait()
        store.start()
    for store in stores:
        store.wait()


def solution(mesh):
    nx, ny = mesh.shape["gx"], mesh.shape["gy"]
    n = nx * ny

    def shards(
        signals, tiles, tile_dir, tile_mask, live_rows, bound_rows, scale_coeffs, spectral_bound
    ):
        ex, ey, chan, size = signals.shape
        slots = tiles.shape[2]
        scales = scale_coeffs.shape[0]
        nb = ex * ey
        width = -(-scales * chan // 128) * 128
        bf, f32 = jnp.bfloat16, jnp.float32
        vmem = pl.BlockSpec(memory_space=pltpu.VMEM)
        hbm = pl.BlockSpec(memory_space=pltpu.HBM)
        made, energy = pl.pallas_call(
            functools.partial(kernel, nx, ny),
            out_shape=(
                jax.ShapeDtypeStruct((scales, ex, ey, chan, size), f32),
                jax.ShapeDtypeStruct((scales, chan), f32),
            ),
            in_specs=[hbm] * 8,
            out_specs=(hbm, vmem),
            scratch_shapes=[
                pltpu.VMEM((scales, ex, ey, chan, size), f32),
                pltpu.VMEM(signals.shape, f32),
                pltpu.SMEM((ex, slots, ey), jnp.int32),
                pltpu.SMEM((ex, slots, ey), jnp.int32),
                pltpu.SMEM((ex, ey), jnp.int32),
                pltpu.SMEM((ex, ey), jnp.int32),
                pltpu.SMEM(scale_coeffs.shape, f32),
                pltpu.SMEM((1, 1), f32),
                pltpu.VMEM((ex, ey, slots, size, size), bf),
                pltpu.VMEM((nb, size, 2 * size), bf),
                pltpu.VMEM((nb, size, size), bf),
                pltpu.VMEM((nb, 2 * chan, size), bf),
                pltpu.VMEM((DEG - 1, nb, chan, size), bf),
                pltpu.VMEM((nb, 2 * chan, size), f32),
                pltpu.VMEM((DEG + 1, nb, chan, size), f32),
                pltpu.VMEM((nb, 1, size), f32),
                pltpu.VMEM((n, 1, width), f32),
                [
                    pltpu.VMEM((ex + 3, ey + 2, chan * (2 if r == 0 else 1), size), bf)
                    for r in range(DEG)
                ],
                pltpu.SemaphoreType.DMA((nb,)),
                pltpu.SemaphoreType.DMA((DEG, 8)),
                pltpu.SemaphoreType.DMA((DEG, 8)),
                pltpu.SemaphoreType.DMA((n,)),
                pltpu.SemaphoreType.DMA((n,)),
                pltpu.SemaphoreType.DMA((8,)),
                pltpu.SemaphoreType.DMA((scales,)),
            ],
            compiler_params=pltpu.CompilerParams(
                collective_id=0, has_side_effects=True, vmem_limit_bytes=VMEM_LIMIT
            ),
        )(
            signals, tiles, jnp.swapaxes(tile_dir, 1, 2), jnp.swapaxes(tile_mask, 1, 2),
            live_rows, bound_rows, scale_coeffs, spectral_bound.reshape(1, 1),
        )
        return pl.pallas_call(
            hand_out,
            out_shape=(
                jax.ShapeDtypeStruct(made.shape, f32), jax.ShapeDtypeStruct(energy.shape, f32)
            ),
            in_specs=[hbm] * 2,
            out_specs=(hbm, hbm),
            scratch_shapes=[
                pltpu.VMEM(made.shape, f32),
                pltpu.VMEM(energy.shape, f32),
                pltpu.SemaphoreType.DMA((scales + 1,)),
                pltpu.SemaphoreType.DMA((scales + 1,)),
            ],
            compiler_params=pltpu.CompilerParams(vmem_limit_bytes=VMEM_LIMIT),
        )(made, energy)

    placed = (
        P("gx", "gy", None, None),
        P("gx", "gy", None, None, None),
        P("gx", "gy", None),
        P("gx", "gy", None),
        P("gx", "gy"),
        P("gx", "gy"),
        P(),
        P(),
    )
    return jax.shard_map(
        shards,
        mesh=mesh,
        in_specs=placed,
        out_specs=(P(None, "gx", "gy", None, None), P()),
        check_vma=False,
    )
```

```python
import functools

import jax
import jax.numpy as jnp
from jax import lax
from jax.experimental import pallas as pl
from jax.experimental.pallas import tpu as pltpu
from jax.sharding import PartitionSpec as P

DEG = 4
VMEM_LIMIT = 67043328
EDGE = 32
MESH = pl.DeviceIdType.MESH
NT = (((1,), (1,)), ((), ()))


def kernel(
    nx, ny, sig_hbm, tiles_hbm, tdir_hbm, tmask_hbm, live_hbm, edge_hbm, coef_hbm, bound_hbm,
    totals_hbm, energy,
    totals, sig, tdir, tmask, live_rows, bound_rows, coef, bound, tiles, w_own, w_edge, own0, own, acc, cheb, slope, en_all, pads, x_out, x_in,
    tile_sem, send_sem, recv_sem, en_send, en_recv, in_sem, out_sem,
):
    ex, ey, chan, size = sig.shape
    slots = tiles.shape[2]
    scales = coef.shape[0]
    groups = size // EDGE
    n = nx * ny
    gx, gy = lax.axis_index("gx"), lax.axis_index("gy")
    me = gx * ny + gy
    blocks = [(i, j) for i in range(ex) for j in range(ey)]

    for r in range(DEG):
        pad = pads[r]
        for row in (0, ex + 1, ex + 2):
            pad[row] = jnp.zeros(pad.shape[1:], pad.dtype)
        for row in range(1, ex + 1):
            for col in (0, ey + 1):
                pad[row, col] = jnp.zeros(pad.shape[2:], pad.dtype)
        x_in[r][...] = jnp.zeros(x_in[r].shape, x_in[r].dtype)

    barrier = pltpu.get_barrier_semaphore()

    fetches = [
        pltpu.make_async_copy(src, dst, in_sem.at[k])
        for k, (src, dst) in enumerate(
            [
                (live_hbm, live_rows), (edge_hbm, bound_rows), (sig_hbm, sig), (tdir_hbm, tdir),
                (tmask_hbm, tmask), (coef_hbm, coef), (bound_hbm, bound),
            ]
        )
    ]
    for copy in fetches:
        copy.start()

    def others(act):
        def one(kx, px, ky):
            py = gy + ky
            act(kx * ny + ky, px, jnp.where(py >= ny, py - ny, py))

        for ky in range(1, ny):
            one(0, gx, ky)

        @pl.loop(1, nx)
        def _(kx):
            px = gx + kx
            px = jnp.where(px >= nx, px - nx, px)
            for ky in range(ny):
                one(kx, px, ky)

    def greet(k, px, py):
        pl.semaphore_signal(barrier, inc=1, device_id=(px, py), device_id_type=MESH)

    others(greet)

    def tile_copy(i, j):
        return pltpu.make_async_copy(
            tiles_hbm.at[i, j], tiles.at[i, j], tile_sem.at[i * ey + j]
        )

    for i, j in blocks:
        tile_copy(i, j).start()

    for copy in fetches:
        copy.wait()

    lane = lax.broadcasted_iota(jnp.int32, (1, size), 1)
    factor = 2.0 / jnp.full((1, size), bound[0, 0], jnp.float32)

    def live_of(i, j):
        return (lane < live_rows[i, j]).astype(jnp.float32)

    def edge_of(i, j):
        return (lane < bound_rows[i, j]).astype(jnp.float32)

    def spread(v, i, j):
        v = v * edge_of(i, j)
        step = EDGE
        while step < size:
            v = v + pltpu.roll(v, step, 1)
            step *= 2
        return v.astype(jnp.bfloat16)

    first_row = lax.broadcasted_iota(jnp.int32, (chan, size), 0) == 0
    for b, (i, j) in enumerate(blocks):
        live = live_of(i, j)
        v = sig[i, j] * live
        cheb[0, b] = v
        ind = jnp.where(first_row, jnp.broadcast_to(live, (chan, size)), 0.0)
        joined = jnp.concatenate([v, ind], axis=0)
        own0[b] = joined.astype(jnp.bfloat16)
        pads[0][i + 1, j + 1] = spread(joined, i, j)

    pl.semaphore_wait(barrier, n - 1)

    sides = []
    for dx in (-1, 0, 1):
        for dy in (-1, 0, 1):
            if dx or dy:
                sides.append((dx, dy))

    def cut(d, extent, far):
        if d == 0:
            return pl.ds(1, extent)
        if far:
            return pl.ds(extent + 1 if d < 0 else 0, 1)
        return pl.ds(1 if d < 0 else extent, 1)

    def inside(dx, dy):
        ok = None
        for d, g, m in ((dx, gx, nx), (dy, gy, ny)):
            if d:
                here = g > 0 if d < 0 else g < m - 1
                ok = here if ok is None else jnp.logical_and(ok, here)
        return ok

    def halo(r, k, dx, dy):
        pad = pads[r]
        if dy == 0:
            src = x_out[r].at[0 if dx < 0 else 1]
            dst = x_in[r].at[1 if dx < 0 else 0]
        else:
            src = pad.at[cut(dx, ex, False), cut(dy, ey, False)]
            dst = pad.at[cut(dx, ex, True), cut(dy, ey, True)]
        return pltpu.make_async_remote_copy(
            src_ref=src,
            dst_ref=dst,
            send_sem=send_sem.at[r, k],
            recv_sem=recv_sem.at[r, k],
            device_id=(gx + dx, gy + dy),
            device_id_type=MESH,
        )

    order = sorted(range(len(sides)), key=lambda k: -abs(sides[k][0]) - abs(sides[k][1]))
    corners = [(i, j) for i, j in blocks if i in (0, ex - 1) and j in (0, ey - 1)]
    inner = [(i, j) for i, j in blocks if (i, j) not in corners]

    def send(r, chosen):
        for k in order:
            dx, dy = sides[k]
            if not chosen(dx, dy):
                continue

            @pl.when(inside(dx, dy))
            def _():
                halo(r, k, dx, dy).start()

    def receive(r):
        for k in order:
            dx, dy = sides[k]

            @pl.when(inside(-dx, -dy))
            def _():
                halo(r, k, dx, dy).wait_recv()

    def group_of(s):
        return jnp.logical_and(lane >= s * EDGE, lane < (s + 1) * EDGE)

    def pack(r, side):
        row = 1 if side == 0 else ex
        for q in range(x_out[r].shape[1]):
            packed = None
            for t in range(min(groups, ey - q * groups)):
                term = pads[r][row, q * groups + t + 1] * group_of(t).astype(jnp.bfloat16)
                packed = term if packed is None else packed + term
            x_out[r][side, q] = packed

    def unpack(r):
        for side in (0, 1):
            for j in range(ey):
                v = x_in[r][side, j // groups].astype(jnp.float32)
                v = jnp.where(group_of(j % groups), v, 0.0)
                step = EDGE
                while step < size:
                    v = v + pltpu.roll(v, step, 1)
                    step *= 2
                pads[r][0 if side == 0 else ex + 1, j + 1] = v.astype(jnp.bfloat16)

    def add_totals(k):
        for s in range(scales):
            c = coef[s, k] * (0.5 if k == 0 else 1.0)
            for b, (i, j) in enumerate(blocks):
                term = c * cheb[k, b]
                totals[s, i, j] = term if k == 0 else totals[s, i, j] + term

    def weights(i, j):
        b = i * ey + j
        total = None
        packed = None
        for s in range(slots):
            tile = tiles[i, j, s].astype(jnp.float32)
            used = jnp.logical_and(tmask[i, s, j] == 1, tdir[i, s, j] == 4)
            term = tile * jnp.where(used, 1.0, 0.0)
            total = term if total is None else total + term
            rolled = pltpu.roll(tile, s * EDGE, 1) if s else tile
            packed = rolled if packed is None else jnp.where(lane >= s * EDGE, rolled, packed)
        high = total.astype(jnp.bfloat16)
        w_own[b, :, :size] = high
        w_own[b, :, size:] = (total - high.astype(jnp.float32)).astype(jnp.bfloat16)
        w_edge[b] = packed.astype(jnp.bfloat16)

    def gather(r, i, j):
        pad = pads[r]
        picked = None
        for s in range(slots):
            d = tdir[i, s, j]
            ok = jnp.logical_and(tmask[i, s, j] == 1, d != 4)
            row = (d * 11) >> 5
            col = d - 3 * row
            cell = pad[jnp.where(ok, row + i, ex + 2), jnp.where(ok, col + j, 0)]
            term = cell * group_of(s).astype(jnp.bfloat16)
            picked = term if picked is None else picked + term
        return picked

    send(0, lambda dx, dy: dy != 0)
    pack(0, 0)
    pack(0, 1)
    send(0, lambda dx, dy: dy == 0)
    for r in range(DEG):
        add_totals(r)
        for b, (i, j) in enumerate(blocks):
            if r == 0:
                tile_copy(i, j).wait()
                weights(i, j)
            mine = own0[b] if r == 0 else own[r - 1, b]
            acc[b, : mine.shape[0]] = lax.dot_general(
                jnp.concatenate([mine, mine], axis=1), w_own[b], NT,
                preferred_element_type=jnp.float32,
            )
        receive(r)
        unpack(r)
        for i, j in corners + inner:
            b = i * ey + j
            rows = 2 * chan if r == 0 else chan
            adj = acc[b, :rows] + lax.dot_general(
                gather(r, i, j), w_edge[b], NT, preferred_element_type=jnp.float32
            )
            scale = factor * live_of(i, j)
            v = cheb[r, b]
            if r == 0:
                slope[b] = scale * adj[chan : chan + 1] - 1.0
                following = slope[b] * v - scale * adj[:chan]
            else:
                following = 2.0 * (slope[b] * v - scale * adj) - cheb[r - 1, b]
            cheb[r + 1, b] = following
            if r < DEG - 1:
                own[r, b] = following.astype(jnp.bfloat16)
                pads[r + 1][i + 1, j + 1] = spread(following, i, j)
                if (i, j) == corners[-1]:
                    send(r + 1, lambda dx, dy: dy and (dx or ex <= 2))
                if (i, j) == inner[-1]:
                    pack(r + 1, 0)
                    pack(r + 1, 1)
                    send(r + 1, lambda dx, dy: not (dy and (dx or ex <= 2)))

    def out_copy(s):
        return pltpu.make_async_copy(totals.at[s], totals_hbm.at[s], out_sem.at[s])

    sums = []
    for s in range(scales):
        c = coef[s, DEG]
        part = jnp.zeros((chan, size), jnp.float32)
        for b, (i, j) in enumerate(blocks):
            t = totals[s, i, j] + c * cheb[DEG, b]
            totals[s, i, j] = t
            part = part + t * t
        sums.append(part)
        out_copy(s).start()

    width = en_all.shape[2]
    if width > scales * chan:
        sums.append(jnp.zeros((width - scales * chan, size), jnp.float32))
    local = lax.dot_general(
        jnp.ones((8, size), jnp.float32), jnp.concatenate(sums, axis=0), NT,
        precision=lax.Precision.HIGHEST, preferred_element_type=jnp.float32,
    )
    en_all[me] = local[:1]

    def share(k, slot, px, py):
        return pltpu.make_async_remote_copy(
            src_ref=en_all.at[slot],
            dst_ref=en_all.at[slot],
            send_sem=en_send.at[k],
            recv_sem=en_recv.at[slot],
            device_id=(px, py),
            device_id_type=MESH,
        )

    others(lambda k, px, py: share(k, me, px, py).start())
    others(lambda k, px, py: share(k, px * ny + py, px, py).wait_recv())

    total = jnp.sum(en_all[...], axis=0) * (1.0 / (ex * ey * size * n))
    for s in range(scales):
        energy[s : s + 1, :] = total[:, s * chan : (s + 1) * chan]

    others(lambda k, px, py: share(k, me, px, py).wait_send())

    for r in range(DEG):
        for k in order:
            dx, dy = sides[k]

            @pl.when(inside(dx, dy))
            def _():
                halo(r, k, dx, dy).wait_send()

    for s in range(scales):
        out_copy(s).wait()


def hand_out(made_hbm, energy_in, out_hbm, energy_out, held, held_energy, load_sem, store_sem):
    count = held.shape[0]
    loads = [
        pltpu.make_async_copy(made_hbm.at[s], held.at[s], load_sem.at[s]) for s in range(count)
    ] + [pltpu.make_async_copy(energy_in, held_energy, load_sem.at[count])]
    stores = [
        pltpu.make_async_copy(held.at[s], out_hbm.at[s], store_sem.at[s]) for s in range(count)
    ] + [pltpu.make_async_copy(held_energy, energy_out, store_sem.at[count])]
    for load in loads:
        load.start()
    for load, store in zip(loads, stores):
        load.wait()
        store.start()
    for store in stores:
        store.wait()


def solution(mesh):
    nx, ny = mesh.shape["gx"], mesh.shape["gy"]
    n = nx * ny

    def shards(
        signals, tiles, tile_dir, tile_mask, live_rows, bound_rows, scale_coeffs, spectral_bound
    ):
        ex, ey, chan, size = signals.shape
        slots = tiles.shape[2]
        scales = scale_coeffs.shape[0]
        nb = ex * ey
        width = -(-scales * chan // 128) * 128
        bf, f32 = jnp.bfloat16, jnp.float32
        vmem = pl.BlockSpec(memory_space=pltpu.VMEM)
        hbm = pl.BlockSpec(memory_space=pltpu.HBM)
        def packed():
            quads = -(-ey * EDGE // size)
            return [
                pltpu.VMEM((2, quads, chan * (2 if r == 0 else 1), size), bf) for r in range(DEG)
            ]

        made, energy = pl.pallas_call(
            functools.partial(kernel, nx, ny),
            out_shape=(
                jax.ShapeDtypeStruct((scales, ex, ey, chan, size), f32),
                jax.ShapeDtypeStruct((scales, chan), f32),
            ),
            in_specs=[hbm] * 8,
            out_specs=(hbm, vmem),
            scratch_shapes=[
                pltpu.VMEM((scales, ex, ey, chan, size), f32),
                pltpu.VMEM(signals.shape, f32),
                pltpu.SMEM((ex, slots, ey), jnp.int32),
                pltpu.SMEM((ex, slots, ey), jnp.int32),
                pltpu.SMEM((ex, ey), jnp.int32),
                pltpu.SMEM((ex, ey), jnp.int32),
                pltpu.SMEM(scale_coeffs.shape, f32),
                pltpu.SMEM((1, 1), f32),
                pltpu.VMEM((ex, ey, slots, size, size), bf),
                pltpu.VMEM((nb, size, 2 * size), bf),
                pltpu.VMEM((nb, size, size), bf),
                pltpu.VMEM((nb, 2 * chan, size), bf),
                pltpu.VMEM((DEG - 1, nb, chan, size), bf),
                pltpu.VMEM((nb, 2 * chan, size), f32),
                pltpu.VMEM((DEG + 1, nb, chan, size), f32),
                pltpu.VMEM((nb, 1, size), f32),
                pltpu.VMEM((n, 1, width), f32),
                [
                    pltpu.VMEM((ex + 3, ey + 2, chan * (2 if r == 0 else 1), size), bf)
                    for r in range(DEG)
                ],
                packed(),
                packed(),
                pltpu.SemaphoreType.DMA((nb,)),
                pltpu.SemaphoreType.DMA((DEG, 8)),
                pltpu.SemaphoreType.DMA((DEG, 8)),
                pltpu.SemaphoreType.DMA((n,)),
                pltpu.SemaphoreType.DMA((n,)),
                pltpu.SemaphoreType.DMA((8,)),
                pltpu.SemaphoreType.DMA((scales,)),
            ],
            compiler_params=pltpu.CompilerParams(
                collective_id=0, has_side_effects=True, vmem_limit_bytes=VMEM_LIMIT
            ),
        )(
            signals, tiles, jnp.swapaxes(tile_dir, 1, 2), jnp.swapaxes(tile_mask, 1, 2),
            live_rows, bound_rows, scale_coeffs, spectral_bound.reshape(1, 1),
        )
        return pl.pallas_call(
            hand_out,
            out_shape=(
                jax.ShapeDtypeStruct(made.shape, f32), jax.ShapeDtypeStruct(energy.shape, f32)
            ),
            in_specs=[hbm] * 2,
            out_specs=(hbm, hbm),
            scratch_shapes=[
                pltpu.VMEM(made.shape, f32),
                pltpu.VMEM(energy.shape, f32),
                pltpu.SemaphoreType.DMA((scales + 1,)),
                pltpu.SemaphoreType.DMA((scales + 1,)),
            ],
            compiler_params=pltpu.CompilerParams(vmem_limit_bytes=VMEM_LIMIT),
        )(made, energy)

    placed = (
        P("gx", "gy", None, None),
        P("gx", "gy", None, None, None),
        P("gx", "gy", None),
        P("gx", "gy", None),
        P("gx", "gy"),
        P("gx", "gy"),
        P(),
        P(),
    )
    return jax.shard_map(
        shards,
        mesh=mesh,
        in_specs=placed,
        out_specs=(P(None, "gx", "gy", None, None), P()),
        check_vma=False,
    )
```
